32 devices in a mesh: row: 8 (over z, y), col: 4 (over x, core).
Axes of the slice: x: 2, y: 2, z: 4, core: 2. Of those that a mesh axis runs over, the one named last changes fastest.
Arguments:
- tracer: float32 [128, 128, 512], P(None, 'row', 'col'), may hold values from -6 to 6
- symbol_x: float32 [128], replicated, may hold values from 0.3 to 3
- symbol_y: float32 [128], replicated, may hold values from 0.3 to 3
- symbol_z: float32 [512], replicated, may hold values from 0.3 to 3
Outputs:
- spectrum: float32 [128, 128, 512], P('row', 'col')
The draws below stay inside these ranges and needn't reach their ends.
All inputs are finite; a program needn't handle non-finite values.
Results may differ from the reference program's by a relative error of at most 0.000075.
Values sent between devices are 32-bit elements; how exact they have to be, the bound alone decides.
No kernel may reach another device: no remote copies, remote signals or barrier semaphores. Data moves between devices by JAX's collectives and lax.ppermute only.
A program may use at most 64 MiB of HBM per device.

```python
import jax
import jax.numpy as jnp
from jax import lax

GRID_X = 128
GRID_Y = 128
GRID_Z = 512


def level_of(stream_key, extent, shards, smallest, largest):
    def one(axis_at, shards_of):
        draws = jax.random.uniform(jax.random.fold_in(jax.random.fold_in(stream_key, 6), axis_at), (shards_of,), jnp.float32, smallest / len(shards), largest / len(shards))
        return jnp.repeat(jnp.exp(draws), extent[axis_at] // shards_of).reshape((-1,) + (1,) * (len(extent) - axis_at - 1))

    level = one(*shards[0])
    for cut in shards[1:]:
        level = level * one(*cut)
    return level


def gaussian(key, dims, deviation, most, cuts=(), dtype=jnp.bfloat16):
    loudness = level_of(key, dims, cuts, -0.22, 0.18) if cuts else 1.0
    values = jax.random.normal(key, dims, jnp.float32) * deviation * loudness
    return jnp.minimum(jnp.maximum(values, -most), most).astype(dtype)


def setup_inputs(seed: int = 0) -> dict:
    seeds = jax.random.split(jax.random.key(seed), 5)
    return {
        "tracer": gaussian(seeds[0], (GRID_X, GRID_Y, GRID_Z), 1.0, 6.0, ((1, 8), (2, 4)), jnp.float32),
        "symbol_x": jnp.clip(jax.random.uniform(seeds[1], (GRID_X,), jnp.float32, 0.3, 3.0), 0.3, 3.0),
        "symbol_y": jnp.clip(jax.random.uniform(seeds[2], (GRID_Y,), jnp.float32, 0.3, 3.0), 0.3, 3.0),
        "symbol_z": jnp.clip(jax.random.uniform(seeds[3], (GRID_Z,), jnp.float32, 0.3, 3.0), 0.3, 3.0),
    }


def transform_table(count):
    rank = jnp.arange(count)
    angle = (jnp.pi / (count + 1)) * (((rank[:, None] + 1) * (rank[None, :] + 1)) % (2 * count + 2)).astype(jnp.float32)
    return jnp.sin(angle) * (2.0 / (count + 1)) ** 0.5


def to_modes(values, dim):
    moved = jnp.tensordot(values, transform_table(values.shape[dim]), axes=([dim], [0]), precision=lax.Precision.HIGHEST)
    return jnp.moveaxis(moved, -1, dim)


def reference(tracer, symbol_x, symbol_y, symbol_z):
    spectrum = tracer
    spectrum = to_modes(spectrum, 0)
    spectrum = to_modes(spectrum, 1)
    spectrum = to_modes(spectrum, 2)
    symbol = symbol_x[:, None, None] + symbol_y[None, :, None] + symbol_z[None, None, :]
    spectrum = spectrum * ((1.0 - 0.2 * symbol) / (1.0 + 0.2 * symbol))
    return spectrum
```

```python
import functools

import jax
import jax.numpy as jnp
import numpy as np
from jax import lax
from jax.experimental import pallas as pl
from jax.experimental.pallas import tpu as pltpu
from jax.sharding import PartitionSpec as P

SPLIT = (8, 8)
GROUP = 4
F32, BF16 = jnp.float32, jnp.bfloat16
VMEM = pl.BlockSpec(memory_space=pltpu.VMEM)
HBM = pl.BlockSpec(memory_space=pltpu.HBM)


def table(count):
    rank = np.arange(1, count + 1, dtype=np.int64)
    angle = np.pi / (count + 1) * (rank[:, None] * rank[None, :] % (2 * count + 2))
    return (np.sin(angle) * (2.0 / (count + 1)) ** 0.5).astype(np.float32)


def halves(values):
    high = values.astype(BF16)
    return high, (values - high.astype(F32)).astype(BF16)


def product(left, right):
    lh, ll = left
    rh, rl = right
    dot = functools.partial(jnp.dot, preferred_element_type=F32)
    return dot(lh, rh) + (dot(ll, rh) + dot(lh, rl))


def call(kernel, outs, flops, ins, out_specs=None, scratch=(), vmem=24 * 2**20, **kw):
    return pl.pallas_call(
        kernel,
        out_shape=outs,
        in_specs=ins,
        out_specs=out_specs if out_specs is not None else [VMEM] * len(outs),
        scratch_shapes=list(scratch),
        compiler_params=pltpu.CompilerParams(vmem_limit_bytes=vmem),
        cost_estimate=pl.CostEstimate(flops=flops, bytes_accessed=0, transcendentals=0),
        **kw,
    )


def sines(left, right, count):
    turns = left.astype(F32) * right.astype(F32)
    period = 2 * count + 2
    turns = turns - jnp.floor(turns * (1.0 / period)) * period - (count + 1)
    return jnp.sin(turns * (-np.pi / (count + 1))) * np.float32((2.0 / (count + 1)) ** 0.5)


def prepare(rows, cols, xh, xl, yh, yl):
    r, c = lax.axis_index("row"), lax.axis_index("col")
    nx, ny = xh.shape[0], yh.shape[0]
    bx, by, bk = nx // rows, ny // rows, ny // cols

    def ramp(count, dim):
        return lax.broadcasted_iota(jnp.int32, (count, 1) if dim == 0 else (1, count), dim)

    across = ramp(nx, 1)
    for d in range(rows):
        at = slice(d * bx, (d + 1) * bx)
        xh[at], xl[at] = halves(sines(ramp(bx, 0) + ((r ^ d) * bx + 1), across + 1, nx))
    across = ramp(ny, 1)
    source = jnp.zeros_like(across)
    for d in range(rows):
        source = jnp.where((across >= d * by) & (across < (d + 1) * by), across + ((r ^ d) * by - d * by + 1), source)
    for e in range(cols):
        at = slice(e * bk, (e + 1) * bk)
        yh[at], yl[at] = halves(sines(ramp(bk, 0) + ((c ^ e) * bk + 1), source, ny))


def x_modes(plan, bx, t_ref, hh_ref, hl_ref, *outs):
    nx, by, bz = t_ref.shape
    left = hh_ref[...], hl_ref[...]
    flat_t = t_ref.reshape(nx * by, bz)
    flat_o = [o.reshape(int(np.prod(o.shape[:-1])), bz) for o in outs]
    for y in range(0, by, 2):
        right = jnp.concatenate([flat_t[pl.ds(y + i, nx, stride=by), :] for i in range(2)], axis=1)
        res = product(left, halves(right))
        for blocks, o in zip(plan, flat_o):
            base = 0
            for d, lo, s in blocks:
                for i in range(2):
                    o[pl.ds(base * by + y + i, s, stride=by), :] = res[d * bx + lo:d * bx + lo + s, i * bz:(i + 1) * bz]
                base += s


def join(keep, came, *outs):
    for h, o in enumerate(outs):
        o[0] = keep[h + 1]
        o[1] = came[h + 1]


def y_modes(places, cols, hh_ref, hl_ref, *refs):
    pieces, outs = refs[:-cols], refs[-cols:]
    s, bk, bz = outs[0].shape
    left = hh_ref[...], hl_ref[...]
    for k in range(0, s, 2):
        ks = range(k, min(k + 2, s))
        right = jnp.concatenate(
            [jnp.concatenate([pieces[i][q] if at is None else pieces[i][at, q] for i, at in places], axis=0) for q in ks], axis=1)
        res = product(left, halves(right))
        for i, q in enumerate(ks):
            for e in range(cols):
                outs[e][q] = res[e * bk:(e + 1) * bk, i * bz:(i + 1) * bz]


def z_part(hh_ref, hl_ref, pieces, es, k0, k1):
    c = lax.axis_index("col")
    _, bk, bz = pieces[0].shape
    left = jnp.concatenate([p[k0:k1].reshape((k1 - k0) * bk, bz) for p in pieces], axis=1)
    ats = [pl.ds(pl.multiple_of((c ^ e) * bz, bz), bz) for e in es]
    right = tuple(jnp.concatenate([h[at, :] for at in ats], axis=0) for h in (hh_ref, hl_ref))
    return product(halves(left), right)


def z_first(lo, half, hh_ref, hl_ref, sx_ref, sy_ref, sz_ref, *refs):
    pieces, (acc, fac, scr_x, scr_y) = refs[:half], refs[half:]
    s, bk, nz = acc.shape
    bx = sx_ref.shape[1] // lax.axis_size("row")
    r, c = lax.axis_index("row"), lax.axis_index("col")
    nx, ny = sx_ref.shape[1], sy_ref.shape[1]
    scr_x[...] = jnp.broadcast_to(sx_ref[...], (128, nx)).T
    scr_y[...] = jnp.broadcast_to(sy_ref[...], (128, ny)).T
    col = scr_y[pl.ds(pl.multiple_of(c * bk, bk), bk), :]
    for k in range(s):
        base = col + scr_x[pl.ds(r * bx + lo + k, 1), :]
        sym = 0.2 * (jnp.concatenate([base] * (nz // 128), axis=1) + sz_ref[...])
        fac[k] = (1.0 - sym) / (1.0 + sym)
    acc[...] = z_part(hh_ref, hl_ref, pieces, list(range(half)), 0, s).reshape(s, bk, nz)


def z_last(lo, half, group, hh_ref, hl_ref, acc, fac, *refs):
    pieces, (out, buf, sems) = refs[:half], refs[-3:]
    s, bk, nz = acc.shape
    copies = []
    for i, k in enumerate(range(0, s, group)):
        e = min(k + group, s)
        part = z_part(hh_ref, hl_ref, pieces, list(range(half, 2 * half)), k, e).reshape(e - k, bk, nz)
        buf[k:e] = (acc[k:e] + part) * fac[k:e]
        copies.append(pltpu.make_async_copy(buf.at[pl.ds(k, e - k)], out.at[pl.ds(lo + k, e - k)], sems.at[i]))
        copies[-1].start()
    for copy in copies:
        copy.wait()


def make(rows, cols):
    def shape(*dims):
        return jax.ShapeDtypeStruct(dims, F32)

    def per_device(tracer, symbol_x, symbol_y, symbol_z):
        nx, by, bz = tracer.shape
        ny, nz = by * rows, bz * cols
        bx, bk = nx // rows, ny // cols
        half = cols // 2
        far, near = range(rows // 2, rows), range(1, rows // 2)
        sizes = [w * bx // 16 for w in SPLIT]
        starts = [sum(sizes[:j]) for j in range(len(sizes))]
        chunks = list(zip(starts, sizes))
        hz = table(nz)
        hzh = hz.astype(jnp.bfloat16)
        hzl = jnp.asarray((hz - hzh.astype(np.float32)).astype(jnp.bfloat16))
        hzh = jnp.asarray(hzh)

        def send(value, axis, d, n):
            return lax.ppermute(value, axis, [(i, i ^ d) for i in range(n)])

        xh, xl, yh, yl = call(
            functools.partial(prepare, rows, cols), [jax.ShapeDtypeStruct((n, n), BF16) for n in (nx, nx, ny, ny)],
            10**9, [])()
        (l0, s0), (l1, s1) = chunks
        deep = rows // 2
        plan = [[(d, l0, s0)] for d in range(rows)]
        plan += [[(2 * h + 1, l1, s1) for h in range(deep)], [(2 * h, l1, s1) for h in range(deep)]]
        u = call(
            functools.partial(x_modes, plan, bx), [shape(s0, by, bz)] * rows + [shape(deep, s1, by, bz)] * 2, 10**8, [VMEM] * 3,
        )(tracer, xh, xl)
        got = {0: u[0]}
        for d in far:
            got[d] = send(u[d], "row", d, rows)
        for d in near:
            got[d] = send(u[d], "row", d, rows)
        keep = u[-1]
        came = send(u[-2], "row", 1, rows)
        both = call(join, [shape(2, s1, by, bz)] * (deep - 1), 10**6, [VMEM] * 2)(keep, came)
        full = [send(both[h - 1], "row", 2 * h, rows) for h in range(1, deep)]

        sx, sy, sz = symbol_x.reshape(1, nx), symbol_y.reshape(1, ny), symbol_z.reshape(1, nz)
        out = None
        for j, (lo, s) in enumerate(chunks):
            if j == 0:
                pieces = [got[d] for d in range(rows)]
                places = [(d, None) for d in range(rows)]
            else:
                pieces = [keep, came] + full
                places = [(0, 0), (1, 0)] + [(2 + h, i) for h in range(deep - 1) for i in range(2)]
            w = call(
                functools.partial(y_modes, places, cols), [shape(s, bk, bz)] * cols,
                10**8, [VMEM] * (2 + len(pieces)))(yh, yl, *pieces)
            w = list(w)
            for e in list(range(half, cols)) + list(range(1, half)):
                w[e] = send(w[e], "col", e, cols)
            acc, fac = call(
                functools.partial(z_first, lo, half), [shape(s, bk, nz)] * 2, 10**8,
                [VMEM] * (5 + half), scratch=[pltpu.VMEM((nx, 128), F32), pltpu.VMEM((ny, 128), F32)],
            )(hzh, hzl, sx, sy, sz, *w[:half])
            prev = [] if out is None else [out]
            out = call(
                functools.partial(z_last, lo, half, GROUP), shape(bx, bk, nz), 10**8,
                [VMEM] * (4 + half) + [HBM] * len(prev), out_specs=HBM,
                scratch=[pltpu.VMEM((s, bk, nz), F32), pltpu.SemaphoreType.DMA((-(-s // GROUP),))],
                input_output_aliases={4 + half: 0} if prev else {},
            )(hzh, hzl, acc, fac, *w[half:], *prev)
        return out

    return per_device


def solution(mesh):
    rows, cols = mesh.shape["row"], mesh.shape["col"]


    body = make(rows, cols)

    in_specs = (P(None, "row", "col"), P(), P(), P())
    return jax.shard_map(body, mesh=mesh, in_specs=in_specs, out_specs=P("row", "col", None), check_vma=False)
```

```python
import functools

import jax
import jax.numpy as jnp
import numpy as np
from jax import lax
from jax.experimental import pallas as pl
from jax.experimental.pallas import tpu as pltpu
from jax.sharding import PartitionSpec as P

SPLIT = (9, 7)
GROUP = 4
F32, BF16 = jnp.float32, jnp.bfloat16
VMEM = pl.BlockSpec(memory_space=pltpu.VMEM)
HBM = pl.BlockSpec(memory_space=pltpu.HBM)


def table(count):
    rank = np.arange(1, count + 1, dtype=np.int64)
    angle = np.pi / (count + 1) * (rank[:, None] * rank[None, :] % (2 * count + 2))
    return (np.sin(angle) * (2.0 / (count + 1)) ** 0.5).astype(np.float32)


def halves(values):
    high = values.astype(BF16)
    return high, (values - high.astype(F32)).astype(BF16)


def product(left, right):
    lh, ll = left
    rh, rl = right
    dot = functools.partial(jnp.dot, preferred_element_type=F32)
    if lh.shape[1] <= 128:
        return dot(jnp.concatenate([lh, ll], axis=1), jnp.concatenate([rh, rh], axis=0)) + dot(lh, rl)
    m = lh.shape[0]
    both = dot(jnp.concatenate([lh, ll], axis=0), rh)
    return both[:m] + (both[m:] + dot(lh, rl))


def call(kernel, outs, flops, ins, out_specs=None, scratch=(), vmem=24 * 2**20, **kw):
    return pl.pallas_call(
        kernel,
        out_shape=outs,
        in_specs=ins,
        out_specs=out_specs if out_specs is not None else [VMEM] * len(outs),
        scratch_shapes=list(scratch),
        compiler_params=pltpu.CompilerParams(vmem_limit_bytes=vmem),
        cost_estimate=pl.CostEstimate(flops=flops, bytes_accessed=0, transcendentals=0),
        **kw,
    )


def sines(left, right, count):
    turns = left.astype(F32) * right.astype(F32)
    period = 2 * count + 2
    turns = turns - jnp.floor(turns * (1.0 / period)) * period - (count + 1)
    return jnp.sin(turns * (-np.pi / (count + 1))) * np.float32((2.0 / (count + 1)) ** 0.5)


def prepare(rows, cols, xh, xl, yh, yl):
    r, c = lax.axis_index("row"), lax.axis_index("col")
    nx, ny = xh.shape[0], yh.shape[0]
    bx, by, bk = nx // rows, ny // rows, ny // cols

    def ramp(count, dim):
        return lax.broadcasted_iota(jnp.int32, (count, 1) if dim == 0 else (1, count), dim)

    across = ramp(nx, 1)
    for d in range(rows):
        at = slice(d * bx, (d + 1) * bx)
        xh[at], xl[at] = halves(sines(ramp(bx, 0) + ((r ^ d) * bx + 1), across + 1, nx))
    across = ramp(ny, 1)
    source = jnp.zeros_like(across)
    for d in range(rows):
        source = jnp.where((across >= d * by) & (across < (d + 1) * by), across + ((r ^ d) * by - d * by + 1), source)
    for e in range(cols):
        at = slice(e * bk, (e + 1) * bk)
        yh[at], yl[at] = halves(sines(ramp(bk, 0) + ((c ^ e) * bk + 1), source, ny))


def x_modes(plan, bx, t_ref, hh_ref, hl_ref, *outs):
    nx, by, bz = t_ref.shape
    left = hh_ref[...], hl_ref[...]
    flat_t = t_ref.reshape(nx * by, bz)
    flat_o = [o.reshape(int(np.prod(o.shape[:-1])), bz) for o in outs]
    for y in range(0, by, 2):
        right = jnp.concatenate([flat_t[pl.ds(y + i, nx, stride=by), :] for i in range(2)], axis=1)
        res = product(left, halves(right))
        for blocks, o in zip(plan, flat_o):
            base = 0
            for d, lo, s in blocks:
                for i in range(2):
                    o[pl.ds(base * by + y + i, s, stride=by), :] = res[d * bx + lo:d * bx + lo + s, i * bz:(i + 1) * bz]
                base += s


def join(keep, came, *outs):
    for h, o in enumerate(outs):
        o[0] = keep[h + 1]
        o[1] = came[h + 1]


def y_modes(places, cols, hh_ref, hl_ref, *refs):
    pieces, outs = refs[:-cols], refs[-cols:]
    s, bk, bz = outs[0].shape
    left = hh_ref[...], hl_ref[...]
    for k in range(0, s, 2):
        ks = range(k, min(k + 2, s))
        right = jnp.concatenate(
            [jnp.concatenate([pieces[i][q] if at is None else pieces[i][at, q] for i, at in places], axis=0) for q in ks], axis=1)
        res = product(left, halves(right))
        for i, q in enumerate(ks):
            for e in range(cols):
                outs[e][q] = res[e * bk:(e + 1) * bk, i * bz:(i + 1) * bz]


def z_part(hh_ref, hl_ref, pieces, es, k0, k1):
    c = lax.axis_index("col")
    _, bk, bz = pieces[0].shape
    left = jnp.concatenate([p[k0:k1].reshape((k1 - k0) * bk, bz) for p in pieces], axis=1)
    ats = [pl.ds(pl.multiple_of((c ^ e) * bz, bz), bz) for e in es]
    right = tuple(jnp.concatenate([h[at, :] for at in ats], axis=0) for h in (hh_ref, hl_ref))
    return product(halves(left), right)


def z_first(lo, half, hh_ref, hl_ref, sx_ref, sy_ref, sz_ref, *refs):
    pieces, (acc, fac, scr_x, scr_y) = refs[:half], refs[half:]
    s, bk, nz = acc.shape
    bx = sx_ref.shape[1] // lax.axis_size("row")
    r, c = lax.axis_index("row"), lax.axis_index("col")
    nx, ny = sx_ref.shape[1], sy_ref.shape[1]
    scr_x[...] = jnp.broadcast_to(sx_ref[...], (128, nx)).T
    scr_y[...] = jnp.broadcast_to(sy_ref[...], (128, ny)).T
    col = scr_y[pl.ds(pl.multiple_of(c * bk, bk), bk), :]
    for k in range(s):
        base = col + scr_x[pl.ds(r * bx + lo + k, 1), :]
        sym = 0.2 * (jnp.concatenate([base] * (nz // 128), axis=1) + sz_ref[...])
        fac[k] = (1.0 - sym) / (1.0 + sym)
    acc[...] = z_part(hh_ref, hl_ref, pieces, list(range(half)), 0, s).reshape(s, bk, nz)


def z_last(lo, half, group, hh_ref, hl_ref, acc, fac, *refs):
    pieces, (out, buf, sems) = refs[:half], refs[-3:]
    s, bk, nz = acc.shape
    copies = []
    for i, k in enumerate(range(0, s, group)):
        e = min(k + group, s)
        part = z_part(hh_ref, hl_ref, pieces, list(range(half, 2 * half)), k, e).reshape(e - k, bk, nz)
        buf[k:e] = (acc[k:e] + part) * fac[k:e]
        copies.append(pltpu.make_async_copy(buf.at[pl.ds(k, e - k)], out.at[pl.ds(lo + k, e - k)], sems.at[i]))
        copies[-1].start()
    for copy in copies:
        copy.wait()


def make(rows, cols):
    def shape(*dims):
        return jax.ShapeDtypeStruct(dims, F32)

    def per_device(tracer, symbol_x, symbol_y, symbol_z):
        nx, by, bz = tracer.shape
        ny, nz = by * rows, bz * cols
        bx, bk = nx // rows, ny // cols
        half = cols // 2
        far, near = range(rows // 2, rows), range(1, rows // 2)
        sizes = [w * bx // 16 for w in SPLIT]
        starts = [sum(sizes[:j]) for j in range(len(sizes))]
        chunks = list(zip(starts, sizes))
        hz = table(nz)
        hzh = hz.astype(jnp.bfloat16)
        hzl = jnp.asarray((hz - hzh.astype(np.float32)).astype(jnp.bfloat16))
        hzh = jnp.asarray(hzh)

        def send(value, axis, d, n):
            return lax.ppermute(value, axis, [(i, i ^ d) for i in range(n)])

        xh, xl, yh, yl = call(
            functools.partial(prepare, rows, cols), [jax.ShapeDtypeStruct((n, n), BF16) for n in (nx, nx, ny, ny)],
            10**9, [])()
        (l0, s0), (l1, s1) = chunks
        deep = rows // 2
        plan = [[(d, l0, s0)] for d in range(rows)]
        plan += [[(2 * h + 1, l1, s1) for h in range(deep)], [(2 * h, l1, s1) for h in range(deep)]]
        u = call(
            functools.partial(x_modes, plan, bx), [shape(s0, by, bz)] * rows + [shape(deep, s1, by, bz)] * 2, 10**8, [VMEM] * 3,
        )(tracer, xh, xl)
        got = {0: u[0]}
        for d in far:
            got[d] = send(u[d], "row", d, rows)
        for d in near:
            got[d] = send(u[d], "row", d, rows)
        keep = u[-1]
        came = send(u[-2], "row", 1, rows)
        both = call(join, [shape(2, s1, by, bz)] * (deep - 1), 10**6, [VMEM] * 2)(keep, came)
        full = [send(both[h - 1], "row", 2 * h, rows) for h in range(1, deep)]

        sx, sy, sz = symbol_x.reshape(1, nx), symbol_y.reshape(1, ny), symbol_z.reshape(1, nz)
        out = None
        for j, (lo, s) in enumerate(chunks):
            if j == 0:
                pieces = [got[d] for d in range(rows)]
                places = [(d, None) for d in range(rows)]
            else:
                pieces = [keep, came] + full
                places = [(0, 0), (1, 0)] + [(2 + h, i) for h in range(deep - 1) for i in range(2)]
            w = call(
                functools.partial(y_modes, places, cols), [shape(s, bk, bz)] * cols,
                10**8, [VMEM] * (2 + len(pieces)))(yh, yl, *pieces)
            w = list(w)
            for e in list(range(half, cols)) + list(range(1, half)):
                w[e] = send(w[e], "col", e, cols)
            acc, fac = call(
                functools.partial(z_first, lo, half), [shape(s, bk, nz)] * 2, 10**8,
                [VMEM] * (5 + half), scratch=[pltpu.VMEM((nx, 128), F32), pltpu.VMEM((ny, 128), F32)],
            )(hzh, hzl, sx, sy, sz, *w[:half])
            prev = [] if out is None else [out]
            out = call(
                functools.partial(z_last, lo, half, GROUP), shape(bx, bk, nz), 10**8,
                [VMEM] * (4 + half) + [HBM] * len(prev), out_specs=HBM,
                scratch=[pltpu.VMEM((s, bk, nz), F32), pltpu.SemaphoreType.DMA((-(-s // GROUP),))],
                input_output_aliases={4 + half: 0} if prev else {},
            )(hzh, hzl, acc, fac, *w[half:], *prev)
        return out

    return per_device


def solution(mesh):
    rows, cols = mesh.shape["row"], mesh.shape["col"]


    body = make(rows, cols)

    in_specs = (P(None, "row", "col"), P(), P(), P())
    return jax.shard_map(body, mesh=mesh, in_specs=in_specs, out_specs=P("row", "col", None), check_vma=False)
```

```python
import functools

import jax
import jax.numpy as jnp
import numpy as np
from jax import lax
from jax.experimental import pallas as pl
from jax.experimental.pallas import tpu as pltpu
from jax.sharding import PartitionSpec as P

SPLIT = (9, 7)
GROUP = 4
F32, BF16 = jnp.float32, jnp.bfloat16
VMEM = pl.BlockSpec(memory_space=pltpu.VMEM)
HBM = pl.BlockSpec(memory_space=pltpu.HBM)


def table(count):
    rank = np.arange(1, count + 1, dtype=np.int64)
    angle = np.pi / (count + 1) * (rank[:, None] * rank[None, :] % (2 * count + 2))
    return (np.sin(angle) * (2.0 / (count + 1)) ** 0.5).astype(np.float32)


def halves(values):
    high = values.astype(BF16)
    return high, (values - high.astype(F32)).astype(BF16)


def product(left, right):
    lh, ll = left
    rh, rl = right
    dot = functools.partial(jnp.dot, preferred_element_type=F32)
    if lh.shape[1] <= 128:
        return dot(jnp.concatenate([lh, ll], axis=1), jnp.concatenate([rh, rh], axis=0)) + dot(lh, rl)
    m = lh.shape[0]
    both = dot(jnp.concatenate([lh, ll], axis=0), rh)
    return both[:m] + (both[m:] + dot(lh, rl))


def call(kernel, outs, flops, ins, out_specs=None, scratch=(), vmem=24 * 2**20, **kw):
    return pl.pallas_call(
        kernel,
        out_shape=outs,
        in_specs=ins,
        out_specs=out_specs if out_specs is not None else [VMEM] * len(outs),
        scratch_shapes=list(scratch),
        compiler_params=pltpu.CompilerParams(vmem_limit_bytes=vmem),
        cost_estimate=pl.CostEstimate(flops=flops, bytes_accessed=0, transcendentals=0),
        **kw,
    )


def sines(left, right, count):
    turns = left.astype(F32) * right.astype(F32)
    period = 2 * count + 2
    turns = turns - jnp.floor(turns * (1.0 / period)) * period - (count + 1)
    return jnp.sin(turns * (-np.pi / (count + 1))) * np.float32((2.0 / (count + 1)) ** 0.5)


def prepare(rows, cols, xh, xl, yh, yl):
    r, c = lax.axis_index("row"), lax.axis_index("col")
    nx, ny = xh.shape[0], yh.shape[0]
    bx, by, bk = nx // rows, ny // rows, ny // cols

    def ramp(count, dim):
        return lax.broadcasted_iota(jnp.int32, (count, 1) if dim == 0 else (1, count), dim)

    across = ramp(nx, 1)
    for d in range(rows):
        at = slice(d * bx, (d + 1) * bx)
        xh[at], xl[at] = halves(sines(ramp(bx, 0) + ((r ^ d) * bx + 1), across + 1, nx))
    across = ramp(ny, 1)
    source = jnp.zeros_like(across)
    for d in range(rows):
        source = jnp.where((across >= d * by) & (across < (d + 1) * by), across + ((r ^ d) * by - d * by + 1), source)
    for e in range(cols):
        at = slice(e * bk, (e + 1) * bk)
        yh[at], yl[at] = halves(sines(ramp(bk, 0) + ((c ^ e) * bk + 1), source, ny))


def x_modes(plan, bx, t_ref, hh_ref, hl_ref, *outs):
    nx, by, bz = t_ref.shape
    left = hh_ref[...], hl_ref[...]
    flat_t = t_ref.reshape(nx * by, bz)
    flat_o = [o.reshape(int(np.prod(o.shape[:-1])), bz) for o in outs]
    for y in range(0, by, 2):
        right = jnp.concatenate([flat_t[pl.ds(y + i, nx, stride=by), :] for i in range(2)], axis=1)
        res = product(left, halves(right))
        for blocks, o in zip(plan, flat_o):
            base = 0
            for d, lo, s in blocks:
                for i in range(2):
                    o[pl.ds(base * by + y + i, s, stride=by), :] = res[d * bx + lo:d * bx + lo + s, i * bz:(i + 1) * bz]
                base += s


def join(keep, came, *outs):
    for h, o in enumerate(outs):
        o[0] = keep[h]
        o[1] = came[h]


def y_modes(places, cols, hh_ref, hl_ref, *refs):
    pieces, outs = refs[:-cols], refs[-cols:]
    s, bk, bz = outs[0].shape
    left = hh_ref[...], hl_ref[...]
    for k in range(0, s, 2):
        ks = range(k, min(k + 2, s))
        right = jnp.concatenate(
            [jnp.concatenate([pieces[i][off + q] if at is None else pieces[i][at, off + q] for i, at, off in places], axis=0) for q in ks], axis=1)
        res = product(left, halves(right))
        for i, q in enumerate(ks):
            for e in range(cols):
                outs[e][q] = res[e * bk:(e + 1) * bk, i * bz:(i + 1) * bz]


def z_part(hh_ref, hl_ref, pieces, es, k0, k1):
    c = lax.axis_index("col")
    _, bk, bz = pieces[0].shape
    left = jnp.concatenate([p[k0:k1].reshape((k1 - k0) * bk, bz) for p in pieces], axis=1)
    ats = [pl.ds(pl.multiple_of((c ^ e) * bz, bz), bz) for e in es]
    right = tuple(jnp.concatenate([h[at, :] for at in ats], axis=0) for h in (hh_ref, hl_ref))
    return product(halves(left), right)


def z_first(lo, half, hh_ref, hl_ref, sx_ref, sy_ref, sz_ref, *refs):
    pieces, (acc, fac, scr_x, scr_y) = refs[:half], refs[half:]
    s, bk, nz = acc.shape
    bx = sx_ref.shape[1] // lax.axis_size("row")
    r, c = lax.axis_index("row"), lax.axis_index("col")
    nx, ny = sx_ref.shape[1], sy_ref.shape[1]
    scr_x[...] = jnp.broadcast_to(sx_ref[...], (128, nx)).T
    scr_y[...] = jnp.broadcast_to(sy_ref[...], (128, ny)).T
    col = scr_y[pl.ds(pl.multiple_of(c * bk, bk), bk), :]
    for k in range(s):
        base = col + scr_x[pl.ds(r * bx + lo + k, 1), :]
        sym = 0.2 * (jnp.concatenate([base] * (nz // 128), axis=1) + sz_ref[...])
        fac[k] = (1.0 - sym) / (1.0 + sym)
    acc[...] = z_part(hh_ref, hl_ref, pieces, list(range(half)), 0, s).reshape(s, bk, nz)


def z_last(lo, half, group, hh_ref, hl_ref, acc, fac, *refs):
    pieces, (out, buf, sems) = refs[:half], refs[-3:]
    s, bk, nz = acc.shape
    copies = []
    for i, k in enumerate(range(0, s, group)):
        e = min(k + group, s)
        part = z_part(hh_ref, hl_ref, pieces, list(range(half, 2 * half)), k, e).reshape(e - k, bk, nz)
        buf[k:e] = (acc[k:e] + part) * fac[k:e]
        copies.append(pltpu.make_async_copy(buf.at[pl.ds(k, e - k)], out.at[pl.ds(lo + k, e - k)], sems.at[i]))
        copies[-1].start()
    for copy in copies:
        copy.wait()


def make(rows, cols):
    def shape(*dims):
        return jax.ShapeDtypeStruct(dims, F32)

    def per_device(tracer, symbol_x, symbol_y, symbol_z):
        nx, by, bz = tracer.shape
        ny, nz = by * rows, bz * cols
        bx, bk = nx // rows, ny // cols
        half = cols // 2
        sizes = [w * bx // 16 for w in SPLIT]
        starts = [sum(sizes[:j]) for j in range(len(sizes))]
        chunks = list(zip(starts, sizes))
        hz = table(nz)
        hzh = hz.astype(jnp.bfloat16)
        hzl = jnp.asarray((hz - hzh.astype(np.float32)).astype(jnp.bfloat16))
        hzh = jnp.asarray(hzh)

        def send(value, axis, d, n):
            return lax.ppermute(value, axis, [(i, i ^ d) for i in range(n)])

        xh, xl, yh, yl = call(
            functools.partial(prepare, rows, cols), [jax.ShapeDtypeStruct((n, n), BF16) for n in (nx, nx, ny, ny)],
            10**9, [])()
        (l0, s0), (l1, s1) = chunks
        deep = rows // 2
        hs = range(1, deep)
        plan = [[(d, 0, bx)] for d in range(2)] + [[(d, l0, s0)] for d in range(2, rows)]
        plan += [[(2 * h + 1, l1, s1) for h in hs], [(2 * h, l1, s1) for h in hs]]
        u = call(
            functools.partial(x_modes, plan, bx),
            [shape(bx, by, bz)] * 2 + [shape(s0, by, bz)] * (rows - 2) + [shape(len(hs), s1, by, bz)] * 2, 10**8,
            [VMEM] * 3)(tracer, xh, xl)
        got = [u[0]] + [send(u[d], "row", d, rows) for d in range(1, rows)]
        keep = u[-1]
        came = send(u[-2], "row", 1, rows)
        both = call(join, [shape(2, s1, by, bz)] * len(hs), 10**6, [VMEM] * 2)(keep, came)
        full = [send(v, "row", 2 * h, rows) for h, v in zip(hs, both)]
        arrived = [(got, [(d, None, 0) for d in range(rows)]),
                   (got[:2] + full, [(d, None, l1) for d in range(2)] + [(2 + h, i, 0) for h in range(len(hs)) for i in range(2)])]

        sx, sy, sz = symbol_x.reshape(1, nx), symbol_y.reshape(1, ny), symbol_z.reshape(1, nz)
        out = None
        for j, (lo, s) in enumerate(chunks):
            pieces, places = arrived[j]
            w = call(
                functools.partial(y_modes, places, cols), [shape(s, bk, bz)] * cols,
                10**8, [VMEM] * (2 + len(pieces)))(yh, yl, *pieces)
            w = list(w)
            for e in list(range(half, cols)) + list(range(1, half)):
                w[e] = send(w[e], "col", e, cols)
            acc, fac = call(
                functools.partial(z_first, lo, half), [shape(s, bk, nz)] * 2, 10**8,
                [VMEM] * (5 + half), scratch=[pltpu.VMEM((nx, 128), F32), pltpu.VMEM((ny, 128), F32)],
            )(hzh, hzl, sx, sy, sz, *w[:half])
            prev = [] if out is None else [out]
            out = call(
                functools.partial(z_last, lo, half, GROUP), shape(bx, bk, nz), 10**8,
                [VMEM] * (4 + half) + [HBM] * len(prev), out_specs=HBM,
                scratch=[pltpu.VMEM((s, bk, nz), F32), pltpu.SemaphoreType.DMA((-(-s // GROUP),))],
                input_output_aliases={4 + half: 0} if prev else {},
            )(hzh, hzl, acc, fac, *w[half:], *prev)
        return out

    return per_device


def solution(mesh):
    rows, cols = mesh.shape["row"], mesh.shape["col"]


    body = make(rows, cols)

    in_specs = (P(None, "row", "col"), P(), P(), P())
    return jax.shard_map(body, mesh=mesh, in_specs=in_specs, out_specs=P("row", "col", None), check_vma=False)
```
